32 devices in a mesh: tm: 4 (over z), mem: 4 (over y, x), tile: 2 (over core).
Axes of the slice: x: 2, y: 2, z: 4, core: 2. Of those that a mesh axis runs over, the one named last changes fastest.
Arguments:
- control: float32 [40, 2, 8, 256], P('mem', None, 'tile'), may hold values from -6 to 6
- vertical_modes: float32 [64, 2], replicated, may hold values from -4 to 4
- mode_counts: int32 [8], P('tile'), may hold values from 1 to 2, as said below
- perturbations: bfloat16 [40, 8, 64, 8, 256], P('mem', 'tm', None, 'tile'), may hold values from -6 to 6
- slot_index: int32 [12], P('tm'), may hold values from 0 to 7, as said below
- blend_weight: float32 [12], P('tm'), may hold values from 0 to 1
Outputs:
- increment: float32 [12, 64, 8, 256], P('tm', None, 'tile')
The draws below stay inside these ranges and needn't reach their ends.
Inputs may be any that keep to these rules, and one draw needn't show every extreme that they name: slot_index[w] // 2 == w // 3. `mode_counts`: both ends of the range occur.
All inputs are finite; a program needn't handle non-finite values.
Results may differ from the reference program's by a relative error of at most 0.0003.
Values sent between devices are 32-bit elements; how exact they have to be, the bound alone decides.
No kernel may reach another device: no remote copies, remote signals or barrier semaphores. Data moves between devices by JAX's collectives and lax.ppermute only.
A program may use at most 64 MiB of HBM per device.

```python
import math
import jax
import jax.numpy as jnp
from jax import lax

LEV = 64
VM = 2
SMOOTH = 4
SLOT_DEV = 2
WIN_DEV = 3
GY = 256
ENS = 40
SLOTS = 8
WIN = 12
NX = 8


def draw_slot_index(key, part):
    blocks = jnp.arange(WIN) // WIN_DEV
    offsets = jax.random.randint(key, (WIN,), 0, SLOT_DEV)
    return (blocks * SLOT_DEV + offsets).astype(jnp.int32)


def draw_mode_counts(key, part):
    first_key = jax.random.fold_in(key, 11)
    second_key = jax.random.fold_in(key, 23)
    counts = jax.random.randint(first_key, (NX,), 1, VM + 1)
    where = jax.random.randint(second_key, (), 0, NX)
    counts = counts.at[where].set(1)
    counts = counts.at[(where + 1) % NX].set(VM)
    return counts.astype(jnp.int32)


def block_scale(stream_key, dims, pieces, smallest, largest):
    gain, own = 1.0, jax.random.fold_in(stream_key, 6)
    for position, parts in pieces:
        steps = jnp.exp(jax.random.uniform(jax.random.fold_in(own, position), (parts,), jnp.float32, smallest / len(pieces), largest / len(pieces)))
        gain = gain * jnp.repeat(steps, dims[position] // parts).reshape([-1 if axis == position else 1 for axis in range(len(dims))])
    return gain


def bell_draw(rng, shape, scale, bound, pieces=(), held_as=jnp.bfloat16):
    array = scale * jax.random.normal(rng, shape, jnp.float32)
    if pieces:
        array = array * block_scale(rng, shape, pieces, -0.22, 0.18)
    return jnp.clip(array, -bound, bound).astype(held_as)


def setup_inputs(seed: int = 0) -> dict:
    splits = jax.random.split(jax.random.key(seed), 7)
    control = bell_draw(splits[0], (ENS, VM, NX, GY), 1.0, 6.0, ((0, 4), (2, 2)), jnp.float32)
    vertical_modes = bell_draw(splits[1], (LEV, VM), 1.0, 4.0, (), jnp.float32)
    mode_counts = draw_mode_counts(jax.random.fold_in(splits[6], 71), 0)
    perturbations = bell_draw(splits[3], (ENS, SLOTS, LEV, NX, GY), 1.0, 6.0, ((0, 4), (1, 4), (3, 2)))
    slot_index = draw_slot_index(jax.random.fold_in(splits[6], 71), 0)
    blend_weight = jnp.clip(1.0 * jax.random.uniform(splits[5], (WIN,), jnp.float32) ** block_scale(splits[5], (WIN,), ((0, 4),), -0.2, 0.2), 0.0, 1.0)
    return dict(control=control, vertical_modes=vertical_modes, mode_counts=mode_counts, perturbations=perturbations, slot_index=slot_index, blend_weight=blend_weight)


diffusion = 0.24

def relax_global(field):
    neighbours = jnp.roll(field, -1, axis=2) + jnp.roll(field, 1, axis=2)
    padded = jnp.pad(field, ((0, 0), (0, 0), (0, 0), (1, 1)))
    lateral = padded[:, :, :, 2:] + padded[:, :, :, :-2]
    return field + diffusion * (neighbours + lateral - 4.0 * field)

def reference(control, vertical_modes, mode_counts, perturbations, slot_index, blend_weight):
    smoothed = control
    for repeat in range(SMOOTH):
        smoothed = relax_global(smoothed)
    localized = jnp.zeros((ENS, LEV, NX, GY), jnp.float32)
    for mode_index in range(VM):
        keep_mode = (mode_index < mode_counts).astype(jnp.float32)
        masked = keep_mode[None, :, None] * smoothed[:, mode_index]
        localized = localized + vertical_modes[:, mode_index][None, :, None, None] * masked[:, None]
    norm_factor = 1.0 / math.sqrt(ENS - 1)
    slots = []
    for slot in range(SLOTS):
        member_total = lax.optimization_barrier(jnp.sum(localized * perturbations[:, slot].astype(jnp.float32), axis=0))
        slots.append(member_total * norm_factor)
    slot_increment = jnp.stack(slots)
    cumulative = jnp.cumsum(slot_increment, axis=0)
    previous = jnp.concatenate([jnp.zeros((1, LEV, NX, GY), jnp.float32), cumulative[:-1]], axis=0)
    weight = blend_weight[:, None, None, None]
    return weight * cumulative[slot_index] + (1.0 - weight) * previous[slot_index]
```

```python
import math

import jax
import jax.numpy as jnp
from jax import lax
from jax.sharding import PartitionSpec as P

VM = 2
SMOOTH = 4

diffusion = 0.24


def ring(count, shift):
    return [(i, (i + shift) % count) for i in range(count)]


def is_power(count):
    return count & (count - 1) == 0


def pairing(count, step):
    if is_power(count):
        return [(i, i ^ step) for i in range(count)]
    return ring(count, step)


def target_of(place, count, step):
    if is_power(count):
        return place ^ step
    return (place + step) % count


def source_of(place, count, step):
    if is_power(count):
        return place ^ step
    return (place - step) % count


def relax(field):
    neighbours = jnp.roll(field, -1, axis=2) + jnp.roll(field, 1, axis=2)
    bordered = jnp.pad(field, ((0, 0), (0, 0), (0, 0), (1, 1)))
    lateral = bordered[:, :, :, 2:] + bordered[:, :, :, :-2]
    return field + diffusion * (neighbours + lateral - 4.0 * field)


def smooth(field):
    count = lax.axis_size("tile")
    width = field.shape[2]
    left = SMOOTH
    while left:
        reach = min(left, width)
        if count == 1:
            wide, start = field, 0
        elif count == 2 and reach == width:
            other = lax.ppermute(field, "tile", ring(2, 1))
            wide, start = jnp.concatenate([field, other], axis=2), 0
        else:
            head = lax.slice_in_dim(field, 0, reach, axis=2)
            tail = lax.slice_in_dim(field, width - reach, width, axis=2)
            before = lax.ppermute(tail, "tile", ring(count, 1))
            after = lax.ppermute(head, "tile", ring(count, -1))
            wide, start = jnp.concatenate([before, field, after], axis=2), reach
        for _ in range(reach):
            wide = relax(wide)
        field = lax.slice_in_dim(wide, start, start + width, axis=2)
        left -= reach
    return field


def per_device(control, vertical_modes, mode_counts, perturbations, slot_index, blend_weight):
    members, slot_count, levels = perturbations.shape[:3]
    group = lax.axis_size("mem")
    place = lax.axis_index("mem")
    share = levels // group
    norm_factor = 1.0 / math.sqrt(members * group - 1)

    field = smooth(control)
    masked = []
    for mode_index in range(VM):
        keep_mode = (mode_index < mode_counts).astype(jnp.float32)
        masked.append(keep_mode[None, :, None] * field[:, mode_index])

    def terms(owner):
        part = lax.dynamic_slice_in_dim(perturbations, owner * share, share, axis=2)
        modes = lax.dynamic_slice_in_dim(vertical_modes, owner * share, share, axis=0)
        localized = sum(
            modes[:, m][None, :, None, None] * masked[m][:, None] for m in range(VM)
        )
        return jnp.sum(localized[:, None] * part.astype(jnp.float32), axis=0)

    arrived = []
    for step in range(group - 1, 0, -1):
        arrived.append(
            lax.ppermute(terms(target_of(place, group, step)), "mem", pairing(group, step))
        )
    slots = terms(place)
    for part in arrived:
        slots = slots + part
    slots = slots * norm_factor

    stages = lax.axis_size("tm")
    stage = lax.axis_index("tm")
    total = jnp.sum(slots, axis=0)
    earlier = jnp.zeros_like(total)
    for step in range(1, stages):
        came = lax.ppermute(total, "tm", ring(stages, step))
        earlier = earlier + jnp.where(stage >= step, came, 0.0)

    local_slot = slot_index - stage * slot_count
    blended = []
    for w in range(slot_index.shape[0]):
        mixed = earlier
        for s in range(slot_count):
            factor = jnp.where(
                local_slot[w] == s, blend_weight[w], jnp.where(local_slot[w] > s, 1.0, 0.0)
            )
            mixed = mixed + factor * slots[s]
        blended.append(mixed)
    blended = jnp.stack(blended)
    return lax.all_gather(blended, "mem", axis=1, tiled=True)


def solution(mesh):
    placed = (
        P("mem", None, "tile", None),
        P(),
        P("tile"),
        P("mem", "tm", None, "tile", None),
        P("tm"),
        P("tm"),
    )
    return jax.shard_map(
        per_device,
        mesh=mesh,
        in_specs=placed,
        out_specs=P("tm", None, "tile", None),
        check_vma=False,
    )
```

```python
import functools
import math

import jax
import jax.numpy as jnp
from jax import lax
from jax.experimental import pallas as pl
from jax.experimental.pallas import tpu as pltpu
from jax.sharding import PartitionSpec as P


SMOOTH = 4
LANES = 128
ROWS = 8
VMEM_BYTES = 64 * 1024 * 1024

diffusion = 0.24


def ring(count, shift):
    return [(i, (i + shift) % count) for i in range(count)]


def is_power(count):
    return count & (count - 1) == 0


def pairing(count, step):
    if is_power(count):
        return [(i, i ^ step) for i in range(count)]
    return ring(count, step)


def target_of(place, count, step):
    if is_power(count):
        return place ^ step
    return lax.rem(place + step, count)


def view(field):
    lead = field.shape[:-3]
    levels, x, y = field.shape[-3:]
    field = field.reshape(*lead, levels, x, y // LANES, LANES)
    field = jnp.swapaxes(field, -3, -2)
    return field.reshape(*lead, levels * x * (y // LANES), LANES)


def unview(rows, x, y):
    lead = rows.shape[:-2]
    tiles = y // LANES
    rows = rows.reshape(*lead, rows.shape[-2] // (x * tiles), tiles, x, LANES)
    rows = jnp.swapaxes(rows, -3, -2)
    return rows.reshape(*lead, -1, x, y)


def relax(field):
    neighbours = jnp.roll(field, -1, axis=2) + jnp.roll(field, 1, axis=2)
    bordered = jnp.pad(field, ((0, 0), (0, 0), (0, 0), (1, 1)))
    lateral = bordered[:, :, :, 2:] + bordered[:, :, :, :-2]
    return field + diffusion * (neighbours + lateral - 4.0 * field)


def smooth(field):
    count = lax.axis_size("tile")
    width = field.shape[2]
    left = SMOOTH
    while left:
        reach = min(left, width)
        head = lax.slice_in_dim(field, 0, reach, axis=2)
        tail = lax.slice_in_dim(field, width - reach, width, axis=2)
        before = lax.ppermute(tail, "tile", ring(count, 1))
        after = lax.ppermute(head, "tile", ring(count, -1))
        wide = jnp.concatenate([before, field, after], axis=2)
        for _ in range(reach):
            wide = relax(wide)
        field = lax.slice_in_dim(wide, reach, reach + width, axis=2)
        left -= reach
    return field


def load_kernel(
    x, modes_hbm, counts_hbm, index_hbm, weight_hbm, own_hbm, part_hbm,
    own_ref, part_ref, splat_ref, mask_ref, factor_ref,
    modes_ref, counts_ref, index_ref, weight_ref, sems,
):
    pairs = [
        (modes_hbm, modes_ref),
        (counts_hbm, counts_ref),
        (index_hbm, index_ref),
        (weight_hbm, weight_ref),
        (own_hbm, own_ref),
        (part_hbm, part_ref),
    ]
    copies = [pltpu.make_async_copy(a, b, sems.at[i]) for i, (a, b) in enumerate(pairs)]
    for copy in copies:
        copy.start()
    for copy in copies[:-2]:
        copy.wait()
    levels, modes = splat_ref.shape[:2]
    for l in range(levels):
        for m in range(modes):
            splat_ref[l, m] = jnp.full((ROWS, LANES), modes_ref[m, l], jnp.float32)
    column = lax.rem(lax.broadcasted_iota(jnp.int32, (ROWS, LANES), 0), x)
    count = jnp.zeros((ROWS, LANES), jnp.int32)
    for i in range(x):
        count = jnp.where(column == i, counts_ref[i], count)
    for m in range(modes):
        mask_ref[m] = (m < count).astype(jnp.float32)
    windows, slots = factor_ref.shape[:2]
    for w in range(windows):
        local = index_ref[w] - lax.axis_index("tm") * slots
        for t in range(slots):
            factor = jnp.where(local == t, weight_ref[w], jnp.where(local > t, 1.0, 0.0))
            factor_ref[w, t] = jnp.full((ROWS, LANES), factor, jnp.float32)
    for copy in copies[-2:]:
        copy.wait()


def smoothed_pair(own, other):
    row = lax.broadcasted_iota(jnp.int32, (ROWS, LANES), 0)
    lane = lax.broadcasted_iota(jnp.int32, (ROWS, LANES), 1)
    half = ROWS // 2
    low = jnp.where(row < half, own, pltpu.roll(other, half, 0))
    high = jnp.where(row < half, pltpu.roll(own, half, 0), other)
    first, last = lane == 0, lane == LANES - 1
    for _ in range(SMOOTH):
        low_up, high_up = pltpu.roll(low, 1, 1), pltpu.roll(high, 1, 1)
        low_down, high_down = pltpu.roll(low, LANES - 1, 1), pltpu.roll(high, LANES - 1, 1)
        low_side = jnp.where(first, 0.0, low_up) + jnp.where(last, high_down, low_down)
        high_side = jnp.where(first, low_up, high_up) + jnp.where(last, 0.0, high_down)
        low_next = pltpu.roll(low, 1, 0) + pltpu.roll(low, ROWS - 1, 0)
        high_next = pltpu.roll(high, 1, 0) + pltpu.roll(high, ROWS - 1, 0)
        low = low + diffusion * (low_next + low_side - 4.0 * low)
        high = high + diffusion * (high_next + high_side - 4.0 * high)
    return jnp.where(row < half, low, pltpu.roll(high, half, 0))


def product(group, step, share, splat_ref, field_ref, part_ref, out_ref):
    members, modes = field_ref.shape[:2]
    slots = part_ref.shape[1]
    owner = target_of(lax.axis_index("mem"), group, step)
    pair = 2 * ROWS
    for j in range(share // 2):
        level = owner * share + 2 * j
        start = pl.multiple_of(level * ROWS, pair)
        localized = []
        for k in range(members):
            halves = []
            for h in range(2):
                value = splat_ref[level + h, 0] * field_ref[k, 0]
                for m in range(1, modes):
                    value = value + splat_ref[level + h, m] * field_ref[k, m]
                halves.append(value)
            localized.append(jnp.concatenate(halves, axis=0))
        for t in range(slots):
            total = None
            for k in range(members):
                term = localized[k] * part_ref[k, t, pl.ds(start, pair), :].astype(jnp.float32)
                total = term if total is None else total + term
            out_ref[t, pl.ds(2 * j * ROWS, pair), :] = total


def smooth_kernel(group, step, share, mask_ref, own_ref, other_ref, splat_ref, part_ref, field_ref, out_ref):
    members, modes = own_ref.shape[:2]
    for k in range(members):
        for m in range(modes):
            field_ref[k, m] = smoothed_pair(own_ref[k, m], other_ref[k, m]) * mask_ref[m]
    product(group, step, share, splat_ref, field_ref, part_ref, out_ref)


def mask_kernel(group, step, share, mask_ref, own_ref, splat_ref, part_ref, field_ref, out_ref):
    members, modes = own_ref.shape[:2]
    for k in range(members):
        for m in range(modes):
            field_ref[k, m] = own_ref[k, m] * mask_ref[m]
    product(group, step, share, splat_ref, field_ref, part_ref, out_ref)


def gather_kernel(norm_factor, *refs):
    *arrived, slots_ref, total_ref = refs
    slots = slots_ref.shape[0]
    whole = None
    for t in range(slots):
        value = arrived[0][t]
        for ref in arrived[1:]:
            value = value + ref[t]
        value = value * norm_factor
        slots_ref[t] = value
        whole = value if whole is None else whole + value
    total_ref[...] = whole


def blend_kernel(factor_ref, slots_ref, *refs):
    *arrived, out_ref = refs
    windows, slots = factor_ref.shape[:2]
    height = slots_ref.shape[1]
    stage = lax.axis_index("tm")
    for r in range(0, height, ROWS):
        rows = slice(r, r + ROWS)
        earlier = None
        for step, ref in enumerate(arrived, 1):
            value = ref[rows] * jnp.where(stage >= step, 1.0, 0.0)
            earlier = value if earlier is None else earlier + value
        for w in range(windows):
            mixed = earlier
            for t in range(slots):
                term = factor_ref[w, t] * slots_ref[t, rows]
                mixed = term if mixed is None else mixed + term
            out_ref[w, rows] = mixed


def place_kernel(height, whole_ref, out_ref, sems):
    owners, windows = whole_ref.shape[:2]
    copies = []
    for i in range(owners):
        for w in range(windows):
            copies.append(
                pltpu.make_async_copy(
                    whole_ref.at[i, w], out_ref.at[w, pl.ds(i * height, height)], sems.at[i, w]
                )
            )
    for copy in copies:
        copy.start()
    for copy in copies:
        copy.wait()


VMEM_SPEC = pl.BlockSpec(memory_space=pltpu.VMEM)
HBM_SPEC = pl.BlockSpec(memory_space=pltpu.HBM)


def call(kernel, arrays, out_shape, cost):
    return pl.pallas_call(
        kernel,
        in_specs=[VMEM_SPEC] * len(arrays),
        out_specs=jax.tree.map(lambda _: VMEM_SPEC, out_shape),
        out_shape=out_shape,
        compiler_params=pltpu.CompilerParams(vmem_limit_bytes=16 * 1024 * 1024),
        cost_estimate=pl.CostEstimate(flops=cost, bytes_accessed=cost, transcendentals=0),
    )(*arrays)


def per_device(control, vertical_modes, mode_counts, perturbations, slot_index, blend_weight):
    members, slot_count, levels, x, y = perturbations.shape
    modes = vertical_modes.shape[1]
    windows = slot_index.shape[0]
    group = lax.axis_size("mem")
    stages = lax.axis_size("tm")
    share = levels // group
    height = share * ROWS
    norm_factor = 1.0 / math.sqrt(members * group - 1)
    f32 = lambda *shape: jax.ShapeDtypeStruct(shape, jnp.float32)
    parts = view(perturbations)
    own = view(control[:, :, None])

    room = parts.size * parts.dtype.itemsize + levels * modes * ROWS * LANES * 4

    loaded, parts, splats, masks, factors = pl.pallas_call(
        functools.partial(load_kernel, x),
        in_specs=[HBM_SPEC] * 6,
        out_specs=[VMEM_SPEC] * 5,
        out_shape=[
            pltpu.VMEM(own.shape, jnp.float32),
            pltpu.VMEM(parts.shape, parts.dtype),
            pltpu.VMEM((levels, modes, ROWS, LANES), jnp.float32),
            pltpu.VMEM((modes, ROWS, LANES), jnp.float32),
            pltpu.VMEM((windows, slot_count, ROWS, LANES), jnp.float32),
        ],
        scratch_shapes=[
            pltpu.SMEM((modes, levels), jnp.float32),
            pltpu.SMEM(mode_counts.shape, jnp.int32),
            pltpu.SMEM(slot_index.shape, jnp.int32),
            pltpu.SMEM(blend_weight.shape, jnp.float32),
            pltpu.SemaphoreType.DMA((6,)),
        ],
        compiler_params=pltpu.CompilerParams(vmem_limit_bytes=VMEM_BYTES - 2 * room),
        cost_estimate=pl.CostEstimate(flops=1000000, bytes_accessed=4000000, transcendentals=0),
    )(vertical_modes.T, mode_counts, slot_index, blend_weight, own, parts)

    def shape_of():
        return f32(slot_count, height, LANES)

    field_shape = f32(members, modes, ROWS, LANES)
    if lax.axis_size("tile") == 2 and x == SMOOTH:
        other = lax.ppermute(control, "tile", ring(2, 1))
        field, first = call(
            functools.partial(smooth_kernel, group, group - 1, share),
            [masks, loaded, view(other[:, :, None]), splats, parts],
            [field_shape, shape_of()],
            2000000,
        )
    else:
        field, first = call(
            functools.partial(mask_kernel, group, group - 1, share),
            [masks, view(smooth(control)[:, :, None]), splats, parts],
            [field_shape, shape_of()],
            2000000,
        )

    def terms(step):
        return call(
            functools.partial(product, group, step, share),
            [splats, field, parts],
            shape_of(),
            1000000,
        )

    arrived = []
    for step in range(group - 1, 0, -1):
        part = first if step == group - 1 else terms(step)
        arrived.append(lax.ppermute(part, "mem", pairing(group, step)))
    slots, total = call(
        functools.partial(gather_kernel, norm_factor),
        [terms(0) if group > 1 else first] + arrived,
        [shape_of(), f32(height, LANES)],
        1000000,
    )

    came = [lax.ppermute(total, "tm", ring(stages, step)) for step in range(1, stages)]
    blended = call(
        blend_kernel, [factors, slots] + came, f32(windows, height, LANES), 1000000
    )
    whole = lax.all_gather(blended, "mem", axis=0, tiled=False)
    placed = pl.pallas_call(
        functools.partial(place_kernel, height),
        in_specs=[VMEM_SPEC],
        out_specs=HBM_SPEC,
        out_shape=f32(windows, levels * ROWS, LANES),
        scratch_shapes=[pltpu.SemaphoreType.DMA((group, windows))],
        compiler_params=pltpu.CompilerParams(vmem_limit_bytes=16 * 1024 * 1024),
    )(whole)
    return unview(placed, x, y)


def solution(mesh):
    placed = (
        P("mem", None, "tile", None),
        P(),
        P("tile"),
        P("mem", "tm", None, "tile", None),
        P("tm"),
        P("tm"),
    )
    return jax.shard_map(
        per_device,
        mesh=mesh,
        in_specs=placed,
        out_specs=P("tm", None, "tile", None),
        check_vma=False,
    )
```

```python
import functools
import math

import jax
import jax.numpy as jnp
from jax import lax
from jax.experimental import pallas as pl
from jax.experimental.pallas import tpu as pltpu
from jax.sharding import PartitionSpec as P


SMOOTH = 4
LANES = 128
ROWS = 8
VMEM_BYTES = 64 * 1024 * 1024

diffusion = 0.24


def ring(count, shift):
    return [(i, (i + shift) % count) for i in range(count)]


def is_power(count):
    return count & (count - 1) == 0


def pairing(count, step):
    if is_power(count):
        return [(i, i ^ step) for i in range(count)]
    return ring(count, step)


def target_of(place, count, step):
    if is_power(count):
        return place ^ step
    return lax.rem(place + step, count)


def view(field):
    lead = field.shape[:-3]
    levels, x, y = field.shape[-3:]
    field = field.reshape(*lead, levels, x, y // LANES, LANES)
    field = jnp.swapaxes(field, -3, -2)
    return field.reshape(*lead, levels * x * (y // LANES), LANES)


def unview(rows, x, y):
    lead = rows.shape[:-2]
    tiles = y // LANES
    rows = rows.reshape(*lead, rows.shape[-2] // (x * tiles), tiles, x, LANES)
    rows = jnp.swapaxes(rows, -3, -2)
    return rows.reshape(*lead, -1, x, y)


def relax(field):
    neighbours = jnp.roll(field, -1, axis=2) + jnp.roll(field, 1, axis=2)
    bordered = jnp.pad(field, ((0, 0), (0, 0), (0, 0), (1, 1)))
    lateral = bordered[:, :, :, 2:] + bordered[:, :, :, :-2]
    return field + diffusion * (neighbours + lateral - 4.0 * field)


def smooth(field):
    count = lax.axis_size("tile")
    width = field.shape[2]
    left = SMOOTH
    while left:
        reach = min(left, width)
        head = lax.slice_in_dim(field, 0, reach, axis=2)
        tail = lax.slice_in_dim(field, width - reach, width, axis=2)
        before = lax.ppermute(tail, "tile", ring(count, 1))
        after = lax.ppermute(head, "tile", ring(count, -1))
        wide = jnp.concatenate([before, field, after], axis=2)
        for _ in range(reach):
            wide = relax(wide)
        field = lax.slice_in_dim(wide, reach, reach + width, axis=2)
        left -= reach
    return field


def load_kernel(
    x, modes_hbm, counts_hbm, index_hbm, weight_hbm, own_hbm, part_hbm,
    own_ref, part_ref, splat_ref, mask_ref, factor_ref,
    modes_ref, counts_ref, index_ref, weight_ref, sems,
):
    pairs = [
        (modes_hbm, modes_ref),
        (counts_hbm, counts_ref),
        (index_hbm, index_ref),
        (weight_hbm, weight_ref),
        (own_hbm, own_ref),
        (part_hbm, part_ref),
    ]
    copies = [pltpu.make_async_copy(a, b, sems.at[i]) for i, (a, b) in enumerate(pairs)]
    for copy in copies:
        copy.start()
    for copy in copies[:-2]:
        copy.wait()
    levels, modes = splat_ref.shape[:2]
    for l in range(levels):
        for m in range(modes):
            splat_ref[l, m] = jnp.full((ROWS, LANES), modes_ref[m, l], jnp.float32)
    column = lax.rem(lax.broadcasted_iota(jnp.int32, (ROWS, LANES), 0), x)
    count = jnp.zeros((ROWS, LANES), jnp.int32)
    for i in range(x):
        count = jnp.where(column == i, counts_ref[i], count)
    for m in range(modes):
        mask_ref[m] = (m < count).astype(jnp.float32)
    windows, slots = factor_ref.shape[:2]
    for w in range(windows):
        local = index_ref[w] - lax.axis_index("tm") * slots
        for t in range(slots):
            factor = jnp.where(local == t, weight_ref[w], jnp.where(local > t, 1.0, 0.0))
            factor_ref[w, t] = jnp.full((ROWS, LANES), factor, jnp.float32)
    for copy in copies[-2:]:
        copy.wait()


def smoothed_pair(own, other):
    row = lax.broadcasted_iota(jnp.int32, (ROWS, LANES), 0)
    lane = lax.broadcasted_iota(jnp.int32, (ROWS, LANES), 1)
    half = ROWS // 2
    low = jnp.where(row < half, own, pltpu.roll(other, half, 0))
    high = jnp.where(row < half, pltpu.roll(own, half, 0), other)
    first, last = lane == 0, lane == LANES - 1
    for _ in range(SMOOTH):
        low_up, high_up = pltpu.roll(low, 1, 1), pltpu.roll(high, 1, 1)
        low_down, high_down = pltpu.roll(low, LANES - 1, 1), pltpu.roll(high, LANES - 1, 1)
        low_side = jnp.where(first, 0.0, low_up) + jnp.where(last, high_down, low_down)
        high_side = jnp.where(first, low_up, high_up) + jnp.where(last, 0.0, high_down)
        low_next = pltpu.roll(low, 1, 0) + pltpu.roll(low, ROWS - 1, 0)
        high_next = pltpu.roll(high, 1, 0) + pltpu.roll(high, ROWS - 1, 0)
        low = low + diffusion * (low_next + low_side - 4.0 * low)
        high = high + diffusion * (high_next + high_side - 4.0 * high)
    return jnp.where(row < half, low, pltpu.roll(high, half, 0))


def product(group, step, share, splat_ref, field_ref, part_ref, total_ref, lead_ref):
    members, modes = field_ref.shape[:2]
    slots = part_ref.shape[1]
    owner = target_of(lax.axis_index("mem"), group, step)
    pair = 2 * ROWS
    for j in range(share // 2):
        level = owner * share + 2 * j
        start = pl.multiple_of(level * ROWS, pair)
        localized = []
        for k in range(members):
            halves = []
            for h in range(2):
                value = splat_ref[level + h, 0] * field_ref[k, 0]
                for m in range(1, modes):
                    value = value + splat_ref[level + h, m] * field_ref[k, m]
                halves.append(value)
            localized.append(jnp.concatenate(halves, axis=0))
        whole = None
        for t in range(slots):
            total = None
            for k in range(members):
                term = localized[k] * part_ref[k, t, pl.ds(start, pair), :].astype(jnp.float32)
                total = term if total is None else total + term
            if t < slots - 1:
                lead_ref[t, pl.ds(2 * j * ROWS, pair), :] = total
            whole = total if whole is None else whole + total
        total_ref[pl.ds(2 * j * ROWS, pair), :] = whole


def smooth_kernel(group, step, share, mask_ref, own_ref, other_ref, splat_ref, part_ref, field_ref, total_ref, lead_ref):
    members, modes = own_ref.shape[:2]
    for k in range(members):
        for m in range(modes):
            field_ref[k, m] = smoothed_pair(own_ref[k, m], other_ref[k, m]) * mask_ref[m]
    product(group, step, share, splat_ref, field_ref, part_ref, total_ref, lead_ref)


def mask_kernel(group, step, share, mask_ref, own_ref, splat_ref, part_ref, field_ref, total_ref, lead_ref):
    members, modes = own_ref.shape[:2]
    for k in range(members):
        for m in range(modes):
            field_ref[k, m] = own_ref[k, m] * mask_ref[m]
    product(group, step, share, splat_ref, field_ref, part_ref, total_ref, lead_ref)


def gather_kernel(norm_factor, *refs):
    *arrived, out_ref = refs
    value = arrived[0][...]
    for ref in arrived[1:]:
        value = value + ref[...]
    out_ref[...] = value * norm_factor


def blend_kernel(norm_factor, parts, factor_ref, total_ref, *refs):
    leads, arrived, out_ref = refs[:parts], refs[parts:-1], refs[-1]
    windows, slots = factor_ref.shape[:2]
    height = total_ref.shape[0]
    stage = lax.axis_index("tm")
    for r in range(0, height, ROWS):
        rows = slice(r, r + ROWS)
        earlier = None
        for step, ref in enumerate(arrived, 1):
            value = ref[rows] * jnp.where(stage >= step, 1.0, 0.0)
            earlier = value if earlier is None else earlier + value
        values, rest = [], total_ref[rows]
        for t in range(slots - 1):
            value = leads[0][t, rows]
            for ref in leads[1:]:
                value = value + ref[t, rows]
            values.append(value * norm_factor)
            rest = rest - values[-1]
        values.append(rest)
        for w in range(windows):
            mixed = earlier
            for t in range(slots):
                term = factor_ref[w, t] * values[t]
                mixed = term if mixed is None else mixed + term
            out_ref[w, rows] = mixed


def place_kernel(height, whole_ref, out_ref, sems):
    owners, windows = whole_ref.shape[:2]
    copies = []
    for i in range(owners):
        for w in range(windows):
            copies.append(
                pltpu.make_async_copy(
                    whole_ref.at[i, w], out_ref.at[w, pl.ds(i * height, height)], sems.at[i, w]
                )
            )
    for copy in copies:
        copy.start()
    for copy in copies:
        copy.wait()


VMEM_SPEC = pl.BlockSpec(memory_space=pltpu.VMEM)
HBM_SPEC = pl.BlockSpec(memory_space=pltpu.HBM)


def call(kernel, arrays, out_shape, cost):
    return pl.pallas_call(
        kernel,
        in_specs=[VMEM_SPEC] * len(arrays),
        out_specs=jax.tree.map(lambda _: VMEM_SPEC, out_shape),
        out_shape=out_shape,
        compiler_params=pltpu.CompilerParams(vmem_limit_bytes=16 * 1024 * 1024),
        cost_estimate=pl.CostEstimate(flops=cost, bytes_accessed=cost, transcendentals=0),
    )(*arrays)


def per_device(control, vertical_modes, mode_counts, perturbations, slot_index, blend_weight):
    members, slot_count, levels, x, y = perturbations.shape
    modes = vertical_modes.shape[1]
    windows = slot_index.shape[0]
    group = lax.axis_size("mem")
    stages = lax.axis_size("tm")
    share = levels // group
    height = share * ROWS
    norm_factor = 1.0 / math.sqrt(members * group - 1)
    f32 = lambda *shape: jax.ShapeDtypeStruct(shape, jnp.float32)
    parts = view(perturbations)
    own = view(control[:, :, None])

    room = parts.size * parts.dtype.itemsize + levels * modes * ROWS * LANES * 4

    loaded, parts, splats, masks, factors = pl.pallas_call(
        functools.partial(load_kernel, x),
        in_specs=[HBM_SPEC] * 6,
        out_specs=[VMEM_SPEC] * 5,
        out_shape=[
            pltpu.VMEM(own.shape, jnp.float32),
            pltpu.VMEM(parts.shape, parts.dtype),
            pltpu.VMEM((levels, modes, ROWS, LANES), jnp.float32),
            pltpu.VMEM((modes, ROWS, LANES), jnp.float32),
            pltpu.VMEM((windows, slot_count, ROWS, LANES), jnp.float32),
        ],
        scratch_shapes=[
            pltpu.SMEM((modes, levels), jnp.float32),
            pltpu.SMEM(mode_counts.shape, jnp.int32),
            pltpu.SMEM(slot_index.shape, jnp.int32),
            pltpu.SMEM(blend_weight.shape, jnp.float32),
            pltpu.SemaphoreType.DMA((6,)),
        ],
        compiler_params=pltpu.CompilerParams(vmem_limit_bytes=VMEM_BYTES - 2 * room),
        cost_estimate=pl.CostEstimate(flops=1000000, bytes_accessed=4000000, transcendentals=0),
    )(vertical_modes.T, mode_counts, slot_index, blend_weight, own, parts)

    shapes = [f32(height, LANES), f32(slot_count - 1, height, LANES)]
    field_shape = f32(members, modes, ROWS, LANES)
    if lax.axis_size("tile") == 2 and x == SMOOTH:
        other = lax.ppermute(control, "tile", ring(2, 1))
        field, *first = call(
            functools.partial(smooth_kernel, group, group - 1, share),
            [masks, loaded, view(other[:, :, None]), splats, parts],
            [field_shape] + shapes,
            2000000,
        )
    else:
        field, *first = call(
            functools.partial(mask_kernel, group, group - 1, share),
            [masks, view(smooth(control)[:, :, None]), splats, parts],
            [field_shape] + shapes,
            2000000,
        )

    products = {group - 1: first}
    for step in range(group - 1):
        products[step] = call(
            functools.partial(product, group, step, share),
            [splats, field, parts],
            shapes,
            1000000,
        )

    totals, leads = [products[0][0]], [products[0][1]]
    for step in range(group - 1, 0, -1):
        totals.append(lax.ppermute(products[step][0], "mem", pairing(group, step)))
    for step in range(group - 1, 0, -1):
        leads.append(lax.ppermute(products[step][1], "mem", pairing(group, step)))
    total = call(functools.partial(gather_kernel, norm_factor), totals, f32(height, LANES), 1000000)

    came = []
    for step in range(1, stages):
        came.append(lax.ppermute(total, "tm", ring(stages, step)))
    blended = call(
        functools.partial(blend_kernel, norm_factor, len(leads)),
        [factors, total] + leads + came,
        f32(windows, height, LANES),
        1000000,
    )
    whole = lax.all_gather(blended, "mem", axis=0, tiled=False)
    placed = pl.pallas_call(
        functools.partial(place_kernel, height),
        in_specs=[VMEM_SPEC],
        out_specs=HBM_SPEC,
        out_shape=f32(windows, levels * ROWS, LANES),
        scratch_shapes=[pltpu.SemaphoreType.DMA((group, windows))],
        compiler_params=pltpu.CompilerParams(vmem_limit_bytes=16 * 1024 * 1024),
    )(whole)
    return unview(placed, x, y)


def solution(mesh):
    placed = (
        P("mem", None, "tile", None),
        P(),
        P("tile"),
        P("mem", "tm", None, "tile", None),
        P("tm"),
        P("tm"),
    )
    return jax.shard_map(
        per_device,
        mesh=mesh,
        in_specs=placed,
        out_specs=P("tm", None, "tile", None),
        check_vma=False,
    )
```

```python
import functools
import math

import jax
import jax.numpy as jnp
from jax import lax
from jax.experimental import pallas as pl
from jax.experimental.pallas import tpu as pltpu
from jax.sharding import PartitionSpec as P


SMOOTH = 4
LANES = 128
ROWS = 8
VMEM_BYTES = 64 * 1024 * 1024

diffusion = 0.24


def ring(count, shift):
    return [(i, (i + shift) % count) for i in range(count)]


def is_power(count):
    return count & (count - 1) == 0


def pairing(count, step):
    if is_power(count):
        return [(i, i ^ step) for i in range(count)]
    return ring(count, step)


def target_of(place, count, step):
    if is_power(count):
        return place ^ step
    return lax.rem(place + step, count)


def far_steps(group):
    return [group - 1] if group > 2 else []


def source_of(place, count, step):
    if is_power(count):
        return place ^ step
    return lax.rem(place - step + count, count)


def view(field):
    lead = field.shape[:-3]
    levels, x, y = field.shape[-3:]
    field = field.reshape(*lead, levels, x, y // LANES, LANES)
    field = jnp.swapaxes(field, -3, -2)
    return field.reshape(*lead, levels * x * (y // LANES), LANES)


def unview(rows, x, y):
    lead = rows.shape[:-2]
    tiles = y // LANES
    rows = rows.reshape(*lead, rows.shape[-2] // (x * tiles), tiles, x, LANES)
    rows = jnp.swapaxes(rows, -3, -2)
    return rows.reshape(*lead, -1, x, y)


def relax(field):
    neighbours = jnp.roll(field, -1, axis=2) + jnp.roll(field, 1, axis=2)
    bordered = jnp.pad(field, ((0, 0), (0, 0), (0, 0), (1, 1)))
    lateral = bordered[:, :, :, 2:] + bordered[:, :, :, :-2]
    return field + diffusion * (neighbours + lateral - 4.0 * field)


def smooth(field):
    count = lax.axis_size("tile")
    width = field.shape[2]
    left = SMOOTH
    while left:
        reach = min(left, width)
        head = lax.slice_in_dim(field, 0, reach, axis=2)
        tail = lax.slice_in_dim(field, width - reach, width, axis=2)
        before = lax.ppermute(tail, "tile", ring(count, 1))
        after = lax.ppermute(head, "tile", ring(count, -1))
        wide = jnp.concatenate([before, field, after], axis=2)
        for _ in range(reach):
            wide = relax(wide)
        field = lax.slice_in_dim(wide, reach, reach + width, axis=2)
        left -= reach
    return field


def load_kernel(
    x, modes_hbm, counts_hbm, index_hbm, weight_hbm, own_hbm, part_hbm,
    own_ref, part_ref, splat_ref, mask_ref, factor_ref,
    modes_ref, counts_ref, index_ref, weight_ref, sems,
):
    pairs = [
        (modes_hbm, modes_ref),
        (counts_hbm, counts_ref),
        (index_hbm, index_ref),
        (weight_hbm, weight_ref),
        (own_hbm, own_ref),
        (part_hbm, part_ref),
    ]
    copies = [pltpu.make_async_copy(a, b, sems.at[i]) for i, (a, b) in enumerate(pairs)]
    for copy in copies:
        copy.start()
    for copy in copies[:-2]:
        copy.wait()
    levels, modes = splat_ref.shape[:2]
    for l in range(levels):
        for m in range(modes):
            splat_ref[l, m] = jnp.full((ROWS, LANES), modes_ref[m, l], jnp.float32)
    column = lax.rem(lax.broadcasted_iota(jnp.int32, (ROWS, LANES), 0), x)
    count = jnp.zeros((ROWS, LANES), jnp.int32)
    for i in range(x):
        count = jnp.where(column == i, counts_ref[i], count)
    for m in range(modes):
        mask_ref[m] = (m < count).astype(jnp.float32)
    windows, slots = factor_ref.shape[:2]
    for w in range(windows):
        local = index_ref[w] - lax.axis_index("tm") * slots
        for t in range(slots):
            factor = jnp.where(local == t, weight_ref[w], jnp.where(local > t, 1.0, 0.0))
            factor_ref[w, t] = jnp.full((ROWS, LANES), factor, jnp.float32)
    for copy in copies[-2:]:
        copy.wait()


def smoothed_pair(own, other):
    row = lax.broadcasted_iota(jnp.int32, (ROWS, LANES), 0)
    lane = lax.broadcasted_iota(jnp.int32, (ROWS, LANES), 1)
    half = ROWS // 2
    low = jnp.where(row < half, own, pltpu.roll(other, half, 0))
    high = jnp.where(row < half, pltpu.roll(own, half, 0), other)
    first, last = lane == 0, lane == LANES - 1
    for _ in range(SMOOTH):
        low_up, high_up = pltpu.roll(low, 1, 1), pltpu.roll(high, 1, 1)
        low_down, high_down = pltpu.roll(low, LANES - 1, 1), pltpu.roll(high, LANES - 1, 1)
        low_side = jnp.where(first, 0.0, low_up) + jnp.where(last, high_down, low_down)
        high_side = jnp.where(first, low_up, high_up) + jnp.where(last, 0.0, high_down)
        low_next = pltpu.roll(low, 1, 0) + pltpu.roll(low, ROWS - 1, 0)
        high_next = pltpu.roll(high, 1, 0) + pltpu.roll(high, ROWS - 1, 0)
        low = low + diffusion * (low_next + low_side - 4.0 * low)
        high = high + diffusion * (high_next + high_side - 4.0 * high)
    return jnp.where(row < half, low, pltpu.roll(high, half, 0))


def product(group, step, share, splat_ref, field_ref, part_ref, total_ref, lead_ref):
    members, modes = field_ref.shape[:2]
    slots = part_ref.shape[1]
    owner = target_of(lax.axis_index("mem"), group, step)
    pair = 2 * ROWS
    for j in range(share // 2):
        level = owner * share + 2 * j
        start = pl.multiple_of(level * ROWS, pair)
        localized = []
        for k in range(members):
            halves = []
            for h in range(2):
                value = splat_ref[level + h, 0] * field_ref[k, 0]
                for m in range(1, modes):
                    value = value + splat_ref[level + h, m] * field_ref[k, m]
                halves.append(value)
            localized.append(jnp.concatenate(halves, axis=0))
        whole = None
        for t in range(slots):
            total = None
            for k in range(members):
                term = localized[k] * part_ref[k, t, pl.ds(start, pair), :].astype(jnp.float32)
                total = term if total is None else total + term
            if t < slots - 1:
                lead_ref[t, pl.ds(2 * j * ROWS, pair), :] = total
            whole = total if whole is None else whole + total
        total_ref[pl.ds(2 * j * ROWS, pair), :] = whole


def smooth_kernel(group, step, share, mask_ref, own_ref, other_ref, splat_ref, part_ref, field_ref, total_ref, lead_ref):
    members, modes = own_ref.shape[:2]
    for k in range(members):
        for m in range(modes):
            field_ref[k, m] = smoothed_pair(own_ref[k, m], other_ref[k, m]) * mask_ref[m]
    product(group, step, share, splat_ref, field_ref, part_ref, total_ref, lead_ref)


def mask_kernel(group, step, share, mask_ref, own_ref, splat_ref, part_ref, field_ref, total_ref, lead_ref):
    members, modes = own_ref.shape[:2]
    for k in range(members):
        for m in range(modes):
            field_ref[k, m] = own_ref[k, m] * mask_ref[m]
    product(group, step, share, splat_ref, field_ref, part_ref, total_ref, lead_ref)


def gather_kernel(norm_factor, *refs):
    *arrived, out_ref = refs
    value = arrived[0][...]
    for ref in arrived[1:]:
        value = value + ref[...]
    out_ref[...] = value * norm_factor


def slots_kernel(norm_factor, total_ref, *refs):
    *leads, slots_ref = refs
    slots = slots_ref.shape[0]
    rest = total_ref[...]
    for t in range(slots - 1):
        value = leads[0][t]
        for ref in leads[1:]:
            value = value + ref[t]
        value = value * norm_factor
        slots_ref[t] = value
        rest = rest - value
    slots_ref[slots - 1] = rest


def mix(factor_ref, slots_ref, earlier, w, rows):
    for t in range(slots_ref.shape[0]):
        earlier = earlier + factor_ref[w, t] * slots_ref[t, rows]
    return earlier


def blend_kernel(stages, factor_ref, slots_ref, *refs):
    *arrived, earlier_ref, out_ref = refs
    windows, height = out_ref.shape[:2]
    stage = lax.axis_index("tm")
    for r in range(0, height, ROWS):
        rows = slice(r, r + ROWS)
        earlier = jnp.zeros((ROWS, LANES), jnp.float32)
        for step, ref in enumerate(arrived, 1):
            source = source_of(stage, stages, step)
            earlier = earlier + ref[rows] * jnp.where(source < stage, 1.0, 0.0)
        earlier_ref[rows] = earlier
        for w in range(windows):
            out_ref[w, rows] = mix(factor_ref, slots_ref, earlier, w, rows)


def copies_out(group, step, part_ref, out_ref, sems):
    windows, height = part_ref.shape[:2]
    owner = source_of(lax.axis_index("mem"), group, step)
    start = pl.multiple_of(owner * height, height)
    return [
        pltpu.make_async_copy(part_ref.at[w], out_ref.at[w, pl.ds(start, height)], sems.at[w])
        for w in range(windows)
    ]


def place_kernel(group, near, far, *refs):
    refs = list(refs)
    if near != [0]:
        refs.pop(0)
    near_refs = [refs.pop(0) for _ in near]
    factor_ref = refs.pop(0) if far else None
    far_refs = [(refs.pop(0), refs.pop(0)) for _ in far]
    out_ref, *parts, sems = refs
    copies = []
    for i, (step, ref) in enumerate(zip(near, near_refs)):
        started = copies_out(group, step, ref, out_ref, sems.at[i])
        for copy in started:
            copy.start()
        copies += started
    for i, (step, (slots_ref, earlier_ref), part_ref) in enumerate(zip(far, far_refs, parts)):
        windows, height = part_ref.shape[:2]
        started = copies_out(group, step, part_ref, out_ref, sems.at[len(near) + i])
        for w in range(windows):
            for r in range(0, height, ROWS):
                rows = slice(r, r + ROWS)
                part_ref[w, rows] = mix(factor_ref, slots_ref, earlier_ref[rows], w, rows)
            started[w].start()
        copies += started
    for copy in copies:
        copy.wait()


VMEM_SPEC = pl.BlockSpec(memory_space=pltpu.VMEM)
HBM_SPEC = pl.BlockSpec(memory_space=pltpu.HBM)


def call(kernel, arrays, out_shape, cost):
    return pl.pallas_call(
        kernel,
        in_specs=[VMEM_SPEC] * len(arrays),
        out_specs=jax.tree.map(lambda _: VMEM_SPEC, out_shape),
        out_shape=out_shape,
        compiler_params=pltpu.CompilerParams(vmem_limit_bytes=16 * 1024 * 1024),
        cost_estimate=pl.CostEstimate(flops=cost, bytes_accessed=cost, transcendentals=0),
    )(*arrays)


def per_device(control, vertical_modes, mode_counts, perturbations, slot_index, blend_weight):
    members, slot_count, levels, x, y = perturbations.shape
    modes = vertical_modes.shape[1]
    windows = slot_index.shape[0]
    group = lax.axis_size("mem")
    stages = lax.axis_size("tm")
    share = levels // group
    height = share * ROWS
    norm_factor = 1.0 / math.sqrt(members * group - 1)
    f32 = lambda *shape: jax.ShapeDtypeStruct(shape, jnp.float32)
    parts = view(perturbations)
    own = view(control[:, :, None])

    room = parts.size * parts.dtype.itemsize + levels * modes * ROWS * LANES * 4

    loaded, parts, splats, masks, factors = pl.pallas_call(
        functools.partial(load_kernel, x),
        in_specs=[HBM_SPEC] * 6,
        out_specs=[VMEM_SPEC] * 5,
        out_shape=[
            pltpu.VMEM(own.shape, jnp.float32),
            pltpu.VMEM(parts.shape, parts.dtype),
            pltpu.VMEM((levels, modes, ROWS, LANES), jnp.float32),
            pltpu.VMEM((modes, ROWS, LANES), jnp.float32),
            pltpu.VMEM((windows, slot_count, ROWS, LANES), jnp.float32),
        ],
        scratch_shapes=[
            pltpu.SMEM((modes, levels), jnp.float32),
            pltpu.SMEM(mode_counts.shape, jnp.int32),
            pltpu.SMEM(slot_index.shape, jnp.int32),
            pltpu.SMEM(blend_weight.shape, jnp.float32),
            pltpu.SemaphoreType.DMA((6,)),
        ],
        compiler_params=pltpu.CompilerParams(vmem_limit_bytes=VMEM_BYTES - 2 * room),
        cost_estimate=pl.CostEstimate(flops=1000000, bytes_accessed=4000000, transcendentals=0),
    )(vertical_modes.T, mode_counts, slot_index, blend_weight, own, parts)

    shapes = [f32(height, LANES), f32(slot_count - 1, height, LANES)]
    field_shape = f32(members, modes, ROWS, LANES)
    if lax.axis_size("tile") == 2 and x == SMOOTH:
        other = lax.ppermute(control, "tile", ring(2, 1))
        field, *first = call(
            functools.partial(smooth_kernel, group, group - 1, share),
            [masks, loaded, view(other[:, :, None]), splats, parts],
            [field_shape] + shapes,
            2000000,
        )
    else:
        field, *first = call(
            functools.partial(mask_kernel, group, group - 1, share),
            [masks, view(smooth(control)[:, :, None]), splats, parts],
            [field_shape] + shapes,
            2000000,
        )

    products = {group - 1: first}
    for step in range(group - 1):
        products[step] = call(
            functools.partial(product, group, step, share),
            [splats, field, parts],
            shapes,
            1000000,
        )

    totals, leads = [products[0][0]], [products[0][1]]
    for step in range(group - 1, 0, -1):
        totals.append(lax.ppermute(products[step][0], "mem", pairing(group, step)))
    for step in range(group - 1, 0, -1):
        leads.append(lax.ppermute(products[step][1], "mem", pairing(group, step)))
    total = call(functools.partial(gather_kernel, norm_factor), totals, f32(height, LANES), 1000000)

    came = []
    for step in range(1, stages):
        came.append(lax.ppermute(total, "tm", pairing(stages, step)))
    slots = call(
        functools.partial(slots_kernel, norm_factor),
        [total] + leads,
        f32(slot_count, height, LANES),
        1000000,
    )
    far = far_steps(group)
    slots_far = {}
    for step in far:
        slots_far[step] = lax.ppermute(slots, "mem", pairing(group, step))
    earlier, blended = call(
        functools.partial(blend_kernel, stages),
        [factors, slots] + came,
        [f32(height, LANES), f32(windows, height, LANES)],
        1000000,
    )
    final = {}
    for step in range(1, group):
        final[step] = lax.ppermute(earlier if step in far else blended, "mem", pairing(group, step))

    def put(near, far, arrays):
        goes_on = near != [0]
        return pl.pallas_call(
            functools.partial(place_kernel, group, near, far),
            in_specs=[HBM_SPEC] * goes_on + [VMEM_SPEC] * (len(arrays) - goes_on),
            out_specs=HBM_SPEC,
            out_shape=pltpu.HBM((windows, levels * ROWS, LANES), jnp.float32),
            scratch_shapes=[pltpu.VMEM((windows, height, LANES), jnp.float32)] * len(far)
            + [pltpu.SemaphoreType.DMA((len(near) + len(far), windows))],
            input_output_aliases={0: 0} if goes_on else {},
            compiler_params=pltpu.CompilerParams(vmem_limit_bytes=16 * 1024 * 1024),
            cost_estimate=pl.CostEstimate(flops=1000000, bytes_accessed=0, transcendentals=0),
        )(*arrays)

    whole = put([0], [], [blended])
    near = [step for step in range(1, group) if step not in far]
    for step in near[:-1]:
        whole = put([step], [], [whole, final[step]])
    if near:
        arrays = [whole, final[near[-1]]] + [factors] * (len(far) > 0)
        for step in far:
            arrays += [slots_far[step], final[step]]
        whole = put(near[-1:], far, arrays)
    return unview(whole, x, y)


def solution(mesh):
    placed = (
        P("mem", None, "tile", None),
        P(),
        P("tile"),
        P("mem", "tm", None, "tile", None),
        P("tm"),
        P("tm"),
    )
    return jax.shard_map(
        per_device,
        mesh=mesh,
        in_specs=placed,
        out_specs=P("tm", None, "tile", None),
        check_vma=False,
    )
```

```python
import functools
import math

import jax
import jax.numpy as jnp
from jax import lax
from jax.experimental import pallas as pl
from jax.experimental.pallas import tpu as pltpu
from jax.sharding import PartitionSpec as P


SMOOTH = 4
LANES = 128
ROWS = 8
VMEM_BYTES = 64 * 1024 * 1024

diffusion = 0.24


def ring(count, shift):
    return [(i, (i + shift) % count) for i in range(count)]


def is_power(count):
    return count & (count - 1) == 0


def pairing(count, step):
    if is_power(count):
        return [(i, i ^ step) for i in range(count)]
    return ring(count, step)


def target_of(place, count, step):
    if is_power(count):
        return place ^ step
    return lax.rem(place + step, count)


def plan_of(group):
    return list(range(group - 1, 0, -1))


def source_of(place, count, step):
    if is_power(count):
        return place ^ step
    return lax.rem(place - step + count, count)


def view(field):
    lead = field.shape[:-3]
    levels, x, y = field.shape[-3:]
    field = field.reshape(*lead, levels, x, y // LANES, LANES)
    field = jnp.swapaxes(field, -3, -2)
    return field.reshape(*lead, levels * x * (y // LANES), LANES)


def unview(rows, x, y):
    lead = rows.shape[:-2]
    tiles = y // LANES
    rows = rows.reshape(*lead, rows.shape[-2] // (x * tiles), tiles, x, LANES)
    rows = jnp.swapaxes(rows, -3, -2)
    return rows.reshape(*lead, -1, x, y)


def relax(field):
    neighbours = jnp.roll(field, -1, axis=2) + jnp.roll(field, 1, axis=2)
    bordered = jnp.pad(field, ((0, 0), (0, 0), (0, 0), (1, 1)))
    lateral = bordered[:, :, :, 2:] + bordered[:, :, :, :-2]
    return field + diffusion * (neighbours + lateral - 4.0 * field)


def smooth(field):
    count = lax.axis_size("tile")
    width = field.shape[2]
    left = SMOOTH
    while left:
        reach = min(left, width)
        head = lax.slice_in_dim(field, 0, reach, axis=2)
        tail = lax.slice_in_dim(field, width - reach, width, axis=2)
        before = lax.ppermute(tail, "tile", ring(count, 1))
        after = lax.ppermute(head, "tile", ring(count, -1))
        wide = jnp.concatenate([before, field, after], axis=2)
        for _ in range(reach):
            wide = relax(wide)
        field = lax.slice_in_dim(wide, reach, reach + width, axis=2)
        left -= reach
    return field


def load_kernel(
    x, modes_hbm, counts_hbm, index_hbm, weight_hbm, own_hbm,
    own_ref, splat_ref, mask_ref, factor_ref,
    modes_ref, counts_ref, index_ref, weight_ref, sems,
):
    pairs = [
        (modes_hbm, modes_ref),
        (counts_hbm, counts_ref),
        (index_hbm, index_ref),
        (weight_hbm, weight_ref),
        (own_hbm, own_ref),
    ]
    copies = [pltpu.make_async_copy(a, b, sems.at[i]) for i, (a, b) in enumerate(pairs)]
    for copy in copies:
        copy.start()
    for copy in copies[:-1]:
        copy.wait()
    levels, modes = splat_ref.shape[:2]
    for l in range(levels):
        for m in range(modes):
            splat_ref[l, m] = jnp.full((ROWS, LANES), modes_ref[m, l], jnp.float32)
    column = lax.rem(lax.broadcasted_iota(jnp.int32, (ROWS, LANES), 0), x)
    count = jnp.zeros((ROWS, LANES), jnp.int32)
    for i in range(x):
        count = jnp.where(column == i, counts_ref[i], count)
    for m in range(modes):
        mask_ref[m] = (m < count).astype(jnp.float32)
    windows, slots = factor_ref.shape[:2]
    for w in range(windows):
        local = index_ref[w] - lax.axis_index("tm") * slots
        for t in range(slots):
            factor = jnp.where(local == t, weight_ref[w], jnp.where(local > t, 1.0, 0.0))
            factor_ref[w, t] = jnp.full((ROWS, LANES), factor, jnp.float32)
    for copy in copies[-1:]:
        copy.wait()


def smoothed_pair(own, other):
    row = lax.broadcasted_iota(jnp.int32, (ROWS, LANES), 0)
    lane = lax.broadcasted_iota(jnp.int32, (ROWS, LANES), 1)
    half = ROWS // 2
    low = jnp.where(row < half, own, pltpu.roll(other, half, 0))
    high = jnp.where(row < half, pltpu.roll(own, half, 0), other)
    first, last = lane == 0, lane == LANES - 1
    for _ in range(SMOOTH):
        low_up, high_up = pltpu.roll(low, 1, 1), pltpu.roll(high, 1, 1)
        low_down, high_down = pltpu.roll(low, LANES - 1, 1), pltpu.roll(high, LANES - 1, 1)
        low_side = jnp.where(first, 0.0, low_up) + jnp.where(last, high_down, low_down)
        high_side = jnp.where(first, low_up, high_up) + jnp.where(last, 0.0, high_down)
        low_next = pltpu.roll(low, 1, 0) + pltpu.roll(low, ROWS - 1, 0)
        high_next = pltpu.roll(high, 1, 0) + pltpu.roll(high, ROWS - 1, 0)
        low = low + diffusion * (low_next + low_side - 4.0 * low)
        high = high + diffusion * (high_next + high_side - 4.0 * high)
    return jnp.where(row < half, low, pltpu.roll(high, half, 0))


def product(group, step, share, splat_ref, field_ref, part_ref, total_ref, lead_ref):
    members, modes = field_ref.shape[:2]
    slots = part_ref.shape[1]
    owner = target_of(lax.axis_index("mem"), group, step)
    pair = 2 * ROWS
    for j in range(share // 2):
        level = owner * share + 2 * j
        start = pl.multiple_of(level * ROWS, pair)
        localized = []
        for k in range(members):
            halves = []
            for h in range(2):
                value = splat_ref[level + h, 0] * field_ref[k, 0]
                for m in range(1, modes):
                    value = value + splat_ref[level + h, m] * field_ref[k, m]
                halves.append(value)
            localized.append(jnp.concatenate(halves, axis=0))
        whole = None
        for t in range(slots):
            total = None
            for k in range(members):
                term = localized[k] * part_ref[k, t, pl.ds(start, pair), :].astype(jnp.float32)
                total = term if total is None else total + term
            if t < slots - 1:
                lead_ref[t, pl.ds(2 * j * ROWS, pair), :] = total
            whole = total if whole is None else whole + total
        total_ref[pl.ds(2 * j * ROWS, pair), :] = whole


def smooth_kernel(mask_ref, own_ref, other_ref, field_ref):
    members, modes = own_ref.shape[:2]
    for k in range(members):
        for m in range(modes):
            field_ref[k, m] = smoothed_pair(own_ref[k, m], other_ref[k, m]) * mask_ref[m]


def mask_kernel(mask_ref, own_ref, field_ref):
    members, modes = own_ref.shape[:2]
    for k in range(members):
        for m in range(modes):
            field_ref[k, m] = own_ref[k, m] * mask_ref[m]


def gather_kernel(norm_factor, *refs):
    *arrived, out_ref = refs
    value = arrived[0][...]
    for ref in arrived[1:]:
        value = value + ref[...]
    out_ref[...] = value * norm_factor


def scale_kernel(norm_factor, lead_ref, out_ref):
    out_ref[...] = lead_ref[...] * norm_factor


def slots_kernel(norm_factor, total_ref, own_ref, *refs):
    *leads, slots_ref = refs
    slots = slots_ref.shape[0]
    rest = total_ref[...]
    for t in range(slots - 1):
        value = own_ref[t]
        for ref in leads:
            value = value + ref[t] * norm_factor
        slots_ref[t] = value
        rest = rest - value
    slots_ref[slots - 1] = rest


def mix_kernel(factor_ref, slots_ref, out_ref):
    windows, height = out_ref.shape[:2]
    for r in range(0, height, ROWS):
        rows = slice(r, r + ROWS)
        for w in range(windows):
            mixed = factor_ref[w, 0] * slots_ref[0, rows]
            for t in range(1, slots_ref.shape[0]):
                mixed = mixed + factor_ref[w, t] * slots_ref[t, rows]
            out_ref[w, rows] = mixed


def earlier_kernel(stages, *refs):
    *arrived, earlier_ref = refs
    stage = lax.axis_index("tm")
    earlier = jnp.zeros(earlier_ref.shape, jnp.float32)
    for step, ref in enumerate(arrived, 1):
        source = source_of(stage, stages, step)
        earlier = earlier + ref[...] * jnp.where(source < stage, 1.0, 0.0)
    earlier_ref[...] = earlier


def copies_out(group, step, part_ref, out_ref, sems):
    windows, height = part_ref.shape[:2]
    owner = source_of(lax.axis_index("mem"), group, step)
    start = pl.multiple_of(owner * height, height)
    return [
        pltpu.make_async_copy(part_ref.at[w], out_ref.at[w, pl.ds(start, height)], sems.at[w])
        for w in range(windows)
    ]


def place_kernel(group, plan, goes_on, factor_ref, *refs):
    refs = list(refs)
    if goes_on:
        refs.pop(0)
    quarters = [(refs.pop(0), refs.pop(0)) for _ in plan]
    out_ref, *parts, sems = refs
    copies = []
    for i, (step, (slots_ref, earlier_ref), part_ref) in enumerate(zip(plan, quarters, parts)):
        windows, height = part_ref.shape[:2]
        started = copies_out(group, step, part_ref, out_ref, sems.at[i])
        for w in range(windows):
            for r in range(0, height, ROWS):
                rows = slice(r, r + ROWS)
                value = earlier_ref[rows]
                if step == 0:
                    value = value + slots_ref[w, rows]
                else:
                    for t in range(slots_ref.shape[0]):
                        value = value + factor_ref[w, t] * slots_ref[t, rows]
                part_ref[w, rows] = value
            started[w].start()
        copies += started
    for copy in copies:
        copy.wait()


VMEM_SPEC = pl.BlockSpec(memory_space=pltpu.VMEM)
HBM_SPEC = pl.BlockSpec(memory_space=pltpu.HBM)


def call(kernel, arrays, out_shape, cost):
    return pl.pallas_call(
        kernel,
        in_specs=[VMEM_SPEC] * len(arrays),
        out_specs=jax.tree.map(lambda _: VMEM_SPEC, out_shape),
        out_shape=out_shape,
        compiler_params=pltpu.CompilerParams(vmem_limit_bytes=16 * 1024 * 1024),
        cost_estimate=pl.CostEstimate(flops=cost, bytes_accessed=cost, transcendentals=0),
    )(*arrays)


def per_device(control, vertical_modes, mode_counts, perturbations, slot_index, blend_weight):
    members, slot_count, levels, x, y = perturbations.shape
    modes = vertical_modes.shape[1]
    windows = slot_index.shape[0]
    group = lax.axis_size("mem")
    stages = lax.axis_size("tm")
    share = levels // group
    height = share * ROWS
    norm_factor = 1.0 / math.sqrt(members * group - 1)
    f32 = lambda *shape: jax.ShapeDtypeStruct(shape, jnp.float32)
    parts = view(perturbations)
    own = view(control[:, :, None])

    room = parts.size * parts.dtype.itemsize + levels * modes * ROWS * LANES * 4

    loaded, splats, masks, factors = pl.pallas_call(
        functools.partial(load_kernel, x),
        in_specs=[HBM_SPEC] * 5,
        out_specs=[VMEM_SPEC] * 4,
        out_shape=[
            pltpu.VMEM(own.shape, jnp.float32),
            pltpu.VMEM((levels, modes, ROWS, LANES), jnp.float32),
            pltpu.VMEM((modes, ROWS, LANES), jnp.float32),
            pltpu.VMEM((windows, slot_count, ROWS, LANES), jnp.float32),
        ],
        scratch_shapes=[
            pltpu.SMEM((modes, levels), jnp.float32),
            pltpu.SMEM(mode_counts.shape, jnp.int32),
            pltpu.SMEM(slot_index.shape, jnp.int32),
            pltpu.SMEM(blend_weight.shape, jnp.float32),
            pltpu.SemaphoreType.DMA((5,)),
        ],
        compiler_params=pltpu.CompilerParams(vmem_limit_bytes=VMEM_BYTES - 2 * room),
        cost_estimate=pl.CostEstimate(flops=1000000000, bytes_accessed=1000000000, transcendentals=0),
    )(vertical_modes.T, mode_counts, slot_index, blend_weight, own)

    shapes = [f32(height, LANES), f32(slot_count - 1, height, LANES)]
    field_shape = f32(members, modes, ROWS, LANES)
    plan = plan_of(group)
    if lax.axis_size("tile") == 2 and x == SMOOTH:
        other = lax.ppermute(control, "tile", ring(2, 1))
        field = call(
            smooth_kernel, [masks, loaded, view(other[:, :, None])], field_shape, 1000
        )
    else:
        field = call(mask_kernel, [masks, view(smooth(control)[:, :, None])], field_shape, 1000)

    products = []
    for step in plan + [0]:
        products.append(
            call(
                functools.partial(product, group, step, share),
                [splats, field, parts],
                shapes,
                1000000,
            )
        )

    totals, leads = [products[-1][0]], [products[-1][1]]
    for i, step in enumerate(plan):
        totals.append(lax.ppermute(products[i][0], "mem", pairing(group, step)))
        leads.append(lax.ppermute(products[i][1], "mem", pairing(group, step)))
    total = call(functools.partial(gather_kernel, norm_factor), totals, f32(height, LANES), 1000000)

    came = []
    for step in range(1, stages):
        came.append(lax.ppermute(total, "tm", pairing(stages, step)))
    scaled = call(
        functools.partial(scale_kernel, norm_factor), [leads[0]], shapes[1], 1000000
    )
    slots = call(
        functools.partial(slots_kernel, norm_factor),
        [total, scaled] + leads[1:],
        f32(slot_count, height, LANES),
        1000000,
    )
    slots_far = []
    for step in plan:
        slots_far.append(lax.ppermute(slots, "mem", pairing(group, step)))
    mixed = call(mix_kernel, [factors, slots], f32(windows, height, LANES), 1000000)
    earlier = call(
        functools.partial(earlier_kernel, stages), came, f32(height, LANES), 1000000
    )
    earlier_far = []
    for step in plan:
        earlier_far.append(lax.ppermute(earlier, "mem", pairing(group, step)))

    def put(steps, whole, quarters):
        first = [] if whole is None else [whole]
        return pl.pallas_call(
            functools.partial(place_kernel, group, steps, bool(first)),
            in_specs=[VMEM_SPEC] + [HBM_SPEC] * len(first) + [VMEM_SPEC] * (2 * len(steps)),
            out_specs=HBM_SPEC,
            out_shape=pltpu.HBM((windows, levels * ROWS, LANES), jnp.float32),
            scratch_shapes=[pltpu.VMEM((windows, height, LANES), jnp.float32)] * len(steps)
            + [pltpu.SemaphoreType.DMA((len(steps), windows))],
            input_output_aliases={1: 0} if first else {},
            compiler_params=pltpu.CompilerParams(vmem_limit_bytes=16 * 1024 * 1024),
            cost_estimate=pl.CostEstimate(flops=1000000, bytes_accessed=0, transcendentals=0),
        )(factors, *first, *[ref for pair in quarters for ref in pair])

    whole = put([0], None, [(mixed, earlier)])
    quarters = list(zip(slots_far, earlier_far))
    if len(plan) > 1:
        whole = put(plan[:1], whole, quarters[:1])
        plan, quarters = plan[1:], quarters[1:]
    if plan:
        whole = put(plan, whole, quarters)
    return unview(whole, x, y)


def solution(mesh):
    placed = (
        P("mem", None, "tile", None),
        P(),
        P("tile"),
        P("mem", "tm", None, "tile", None),
        P("tm"),
        P("tm"),
    )
    return jax.shard_map(
        per_device,
        mesh=mesh,
        in_specs=placed,
        out_specs=P("tm", None, "tile", None),
        check_vma=False,
    )
```

```python
import functools
import math

import jax
import jax.numpy as jnp
from jax import lax
from jax.experimental import pallas as pl
from jax.experimental.pallas import tpu as pltpu
from jax.sharding import PartitionSpec as P


SMOOTH = 4
LANES = 128
ROWS = 8
VMEM_BYTES = 64 * 1024 * 1024

diffusion = 0.24


def ring(count, shift):
    return [(i, (i + shift) % count) for i in range(count)]


def is_power(count):
    return count & (count - 1) == 0


def pairing(count, step):
    if is_power(count):
        return [(i, i ^ step) for i in range(count)]
    return ring(count, step)


def target_of(place, count, step):
    if is_power(count):
        return place ^ step
    return lax.rem(place + step, count)


def plan_of(group):
    return list(range(group - 1, 0, -1))


def source_of(place, count, step):
    if is_power(count):
        return place ^ step
    return lax.rem(place - step + count, count)


def view(field):
    lead = field.shape[:-3]
    levels, x, y = field.shape[-3:]
    field = field.reshape(*lead, levels, x, y // LANES, LANES)
    field = jnp.swapaxes(field, -3, -2)
    return field.reshape(*lead, levels * x * (y // LANES), LANES)


def flat(field):
    return view(field.reshape(-1, *field.shape[2:]))


def unview(rows, x, y):
    lead = rows.shape[:-2]
    tiles = y // LANES
    rows = rows.reshape(*lead, rows.shape[-2] // (x * tiles), tiles, x, LANES)
    rows = jnp.swapaxes(rows, -3, -2)
    return rows.reshape(*lead, -1, x, y)


def relax(field):
    neighbours = jnp.roll(field, -1, axis=2) + jnp.roll(field, 1, axis=2)
    bordered = jnp.pad(field, ((0, 0), (0, 0), (0, 0), (1, 1)))
    lateral = bordered[:, :, :, 2:] + bordered[:, :, :, :-2]
    return field + diffusion * (neighbours + lateral - 4.0 * field)


def smooth(field):
    count = lax.axis_size("tile")
    width = field.shape[2]
    left = SMOOTH
    while left:
        reach = min(left, width)
        head = lax.slice_in_dim(field, 0, reach, axis=2)
        tail = lax.slice_in_dim(field, width - reach, width, axis=2)
        before = lax.ppermute(tail, "tile", ring(count, 1))
        after = lax.ppermute(head, "tile", ring(count, -1))
        wide = jnp.concatenate([before, field, after], axis=2)
        for _ in range(reach):
            wide = relax(wide)
        field = lax.slice_in_dim(wide, reach, reach + width, axis=2)
        left -= reach
    return field


def load_kernel(
    x, modes_hbm, counts_hbm, index_hbm, weight_hbm, own_hbm,
    own_ref, splat_ref, mask_ref, factor_ref,
    modes_ref, counts_ref, index_ref, weight_ref, sems,
):
    pairs = [
        (modes_hbm, modes_ref),
        (counts_hbm, counts_ref),
        (index_hbm, index_ref),
        (weight_hbm, weight_ref),
        (own_hbm, own_ref),
    ]
    copies = [pltpu.make_async_copy(a, b, sems.at[i]) for i, (a, b) in enumerate(pairs)]
    for copy in copies:
        copy.start()
    for copy in copies[:-1]:
        copy.wait()
    levels, modes = splat_ref.shape[:2]
    for l in range(levels):
        for m in range(modes):
            splat_ref[l, m] = jnp.full((ROWS, LANES), modes_ref[m, l], jnp.float32)
    mode = lax.rem(lax.broadcasted_iota(jnp.int32, mask_ref.shape[1:], 0), modes)
    for i in range(x):
        mask_ref[i] = (mode < counts_ref[i]).astype(jnp.float32)
    windows, slots = factor_ref.shape[:2]
    for w in range(windows):
        local = index_ref[w] - lax.axis_index("tm") * slots
        for t in range(slots):
            factor = jnp.where(local == t, weight_ref[w], jnp.where(local > t, 1.0, 0.0))
            factor_ref[w, t] = jnp.full((ROWS, LANES), factor, jnp.float32)
    for copy in copies[-1:]:
        copy.wait()


def product(group, step, share, splat_ref, field_ref, part_ref, total_ref, lead_ref):
    members, slots = part_ref.shape[:2]
    modes = splat_ref.shape[1]
    owner = target_of(lax.axis_index("mem"), group, step)
    pair = 2 * ROWS
    for j in range(share // 2):
        level = owner * share + 2 * j
        start = pl.multiple_of(level * ROWS, pair)
        localized = []
        for k in range(members):
            halves = []
            for h in range(2):
                value = splat_ref[level + h, 0] * field_ref[pl.ds(k * modes * ROWS, ROWS), :]
                for m in range(1, modes):
                    value = value + splat_ref[level + h, m] * field_ref[pl.ds((k * modes + m) * ROWS, ROWS), :]
                halves.append(value)
            localized.append(jnp.concatenate(halves, axis=0))
        whole = None
        for t in range(slots):
            total = None
            for k in range(members):
                term = localized[k] * part_ref[k, t, pl.ds(start, pair), :].astype(jnp.float32)
                total = term if total is None else total + term
            if t < slots - 1:
                lead_ref[t, pl.ds(2 * j * ROWS, pair), :] = total
            whole = total if whole is None else whole + total
        total_ref[pl.ds(2 * j * ROWS, pair), :] = whole


def smooth_kernel(mask_ref, own_ref, other_ref, field_ref):
    x, pairs = mask_ref.shape[:2]
    tiles = ROWS // x
    cells = [
        [ref[pl.ds(tile * x + i, pairs, stride=ROWS), :] for tile in range(tiles)]
        for ref in (own_ref, other_ref)
        for i in range(x)
    ]
    lane = lax.broadcasted_iota(jnp.int32, (pairs, LANES), 1)
    first, last = lane == 0, lane == LANES - 1
    round_ = len(cells)
    for left in range(SMOOTH - 1, -1, -1):
        fresh = list(cells)
        for i in sorted({j % round_ for j in range(-left, x + left)}):
            up = [pltpu.roll(part, 1, 1) for part in cells[i]]
            down = [pltpu.roll(part, LANES - 1, 1) for part in cells[i]]
            fresh[i] = []
            for tile in range(tiles):
                before = up[tile - 1] if tile else 0.0
                after = down[tile + 1] if tile + 1 < tiles else 0.0
                near = jnp.where(first, before, up[tile]) + jnp.where(last, after, down[tile])
                near = near + (cells[i - 1][tile] + cells[(i + 1) % round_][tile])
                fresh[i].append((1.0 - 4.0 * diffusion) * cells[i][tile] + diffusion * near)
        cells = fresh
    for i in range(x):
        for tile in range(tiles):
            field_ref[pl.ds(tile * x + i, pairs, stride=ROWS), :] = cells[i][tile] * mask_ref[i]


def mask_kernel(mask_ref, own_ref, field_ref):
    x, pairs = mask_ref.shape[:2]
    for i in range(ROWS):
        rows = pl.ds(i, pairs, stride=ROWS)
        field_ref[rows, :] = own_ref[rows, :] * mask_ref[i % x]


def gather_kernel(norm_factor, *refs):
    *arrived, out_ref = refs
    value = arrived[0][...]
    for ref in arrived[1:]:
        value = value + ref[...]
    out_ref[...] = value * norm_factor


def scale_kernel(norm_factor, lead_ref, out_ref):
    out_ref[...] = lead_ref[...] * norm_factor


def slots_kernel(norm_factor, total_ref, own_ref, *refs):
    *leads, slots_ref = refs
    slots = slots_ref.shape[0]
    rest = total_ref[...]
    for t in range(slots - 1):
        value = own_ref[t]
        for ref in leads:
            value = value + ref[t] * norm_factor
        slots_ref[t] = value
        rest = rest - value
    slots_ref[slots - 1] = rest


def mix_kernel(factor_ref, slots_ref, out_ref):
    windows, height = out_ref.shape[:2]
    for r in range(0, height, ROWS):
        rows = slice(r, r + ROWS)
        for w in range(windows):
            mixed = factor_ref[w, 0] * slots_ref[0, rows]
            for t in range(1, slots_ref.shape[0]):
                mixed = mixed + factor_ref[w, t] * slots_ref[t, rows]
            out_ref[w, rows] = mixed


def earlier_kernel(stages, *refs):
    *arrived, earlier_ref = refs
    stage = lax.axis_index("tm")
    earlier = jnp.zeros(earlier_ref.shape, jnp.float32)
    for step, ref in enumerate(arrived, 1):
        source = source_of(stage, stages, step)
        earlier = earlier + ref[...] * jnp.where(source < stage, 1.0, 0.0)
    earlier_ref[...] = earlier


def copies_out(group, step, part_ref, out_ref, sems):
    windows, height = part_ref.shape[:2]
    owner = source_of(lax.axis_index("mem"), group, step)
    start = pl.multiple_of(owner * height, height)
    return [
        pltpu.make_async_copy(part_ref.at[w], out_ref.at[w, pl.ds(start, height)], sems.at[w])
        for w in range(windows)
    ]


def place_kernel(group, plan, goes_on, *refs):
    refs = list(refs)
    if goes_on:
        refs.pop(0)
    quarters = [(refs.pop(0), refs.pop(0)) for _ in plan]
    out_ref, *parts, sems = refs
    copies = []
    for i, (step, (mixed_ref, earlier_ref), part_ref) in enumerate(zip(plan, quarters, parts)):
        started = copies_out(group, step, part_ref, out_ref, sems.at[i])
        for w, copy in enumerate(started):
            part_ref[w] = mixed_ref[w] + earlier_ref[...]
            copy.start()
        copies += started
    for copy in copies:
        copy.wait()


VMEM_SPEC = pl.BlockSpec(memory_space=pltpu.VMEM)
HBM_SPEC = pl.BlockSpec(memory_space=pltpu.HBM)


def call(kernel, arrays, out_shape, cost):
    return pl.pallas_call(
        kernel,
        in_specs=[VMEM_SPEC] * len(arrays),
        out_specs=jax.tree.map(lambda _: VMEM_SPEC, out_shape),
        out_shape=out_shape,
        compiler_params=pltpu.CompilerParams(vmem_limit_bytes=16 * 1024 * 1024),
        cost_estimate=pl.CostEstimate(flops=cost, bytes_accessed=cost, transcendentals=0),
    )(*arrays)


def per_device(control, vertical_modes, mode_counts, perturbations, slot_index, blend_weight):
    members, slot_count, levels, x, y = perturbations.shape
    modes = vertical_modes.shape[1]
    windows = slot_index.shape[0]
    group = lax.axis_size("mem")
    stages = lax.axis_size("tm")
    share = levels // group
    height = share * ROWS
    norm_factor = 1.0 / math.sqrt(members * group - 1)
    f32 = lambda *shape: jax.ShapeDtypeStruct(shape, jnp.float32)
    parts = view(perturbations)
    own = flat(control)

    room = parts.size * parts.dtype.itemsize + levels * modes * ROWS * LANES * 4

    loaded, splats, masks, factors = pl.pallas_call(
        functools.partial(load_kernel, x),
        in_specs=[HBM_SPEC] * 5,
        out_specs=[VMEM_SPEC] * 4,
        out_shape=[
            pltpu.VMEM(own.shape, jnp.float32),
            pltpu.VMEM((levels, modes, ROWS, LANES), jnp.float32),
            pltpu.VMEM((x, members * modes, LANES), jnp.float32),
            pltpu.VMEM((windows, slot_count, ROWS, LANES), jnp.float32),
        ],
        scratch_shapes=[
            pltpu.SMEM((modes, levels), jnp.float32),
            pltpu.SMEM(mode_counts.shape, jnp.int32),
            pltpu.SMEM(slot_index.shape, jnp.int32),
            pltpu.SMEM(blend_weight.shape, jnp.float32),
            pltpu.SemaphoreType.DMA((5,)),
        ],
        compiler_params=pltpu.CompilerParams(vmem_limit_bytes=VMEM_BYTES - 2 * room),
        cost_estimate=pl.CostEstimate(flops=1000000000, bytes_accessed=1000000000, transcendentals=0),
    )(vertical_modes.T, mode_counts, slot_index, blend_weight, own)

    shapes = [f32(height, LANES), f32(slot_count - 1, height, LANES)]
    field_shape = f32(members * modes * ROWS, LANES)
    plan = plan_of(group)
    if lax.axis_size("tile") == 2 and x == SMOOTH:
        other = lax.ppermute(control, "tile", ring(2, 1))
        field = call(
            smooth_kernel, [masks, loaded, flat(other)], field_shape, 1000
        )
    else:
        field = call(mask_kernel, [masks, flat(smooth(control))], field_shape, 1000)

    products = []
    for step in plan + [0]:
        products.append(
            call(
                functools.partial(product, group, step, share),
                [splats, field, parts],
                shapes,
                1000000,
            )
        )

    totals, leads = [products[-1][0]], [products[-1][1]]
    for i, step in enumerate(plan):
        totals.append(lax.ppermute(products[i][0], "mem", pairing(group, step)))
        leads.append(lax.ppermute(products[i][1], "mem", pairing(group, step)))
    total = call(functools.partial(gather_kernel, norm_factor), totals, f32(height, LANES), 1000000)

    came = []
    for step in range(1, stages):
        came.append(lax.ppermute(total, "tm", pairing(stages, step)))
    scaled = call(
        functools.partial(scale_kernel, norm_factor), [leads[0]], shapes[1], 1000000
    )
    slots = call(
        functools.partial(slots_kernel, norm_factor),
        [total, scaled] + leads[1:],
        f32(slot_count, height, LANES),
        1000000,
    )
    slots_far = []
    for step in plan:
        slots_far.append(lax.ppermute(slots, "mem", pairing(group, step)))
    mixed = call(mix_kernel, [factors, slots], f32(windows, height, LANES), 1000000)
    earlier = call(
        functools.partial(earlier_kernel, stages), came, f32(height, LANES), 1000000
    )
    earlier_far = []
    for step in plan:
        earlier_far.append(lax.ppermute(earlier, "mem", pairing(group, step)))

    def put(steps, whole, quarters):
        first = [] if whole is None else [whole]
        return pl.pallas_call(
            functools.partial(place_kernel, group, steps, bool(first)),
            in_specs=[HBM_SPEC] * len(first) + [VMEM_SPEC] * (2 * len(steps)),
            out_specs=HBM_SPEC,
            out_shape=pltpu.HBM((windows, levels * ROWS, LANES), jnp.float32),
            scratch_shapes=[pltpu.VMEM((windows, height, LANES), jnp.float32)] * len(steps)
            + [pltpu.SemaphoreType.DMA((len(steps), windows))],
            input_output_aliases={0: 0} if first else {},
            compiler_params=pltpu.CompilerParams(vmem_limit_bytes=16 * 1024 * 1024),
            cost_estimate=pl.CostEstimate(flops=1000000, bytes_accessed=0, transcendentals=0),
        )(*first, *[ref for pair in quarters for ref in pair])

    whole = put([0], None, [(mixed, earlier)])
    quarters = []
    for i, part in enumerate(slots_far):
        part = call(mix_kernel, [factors, part], f32(windows, height, LANES), 1000000)
        quarters.append((part, earlier_far[i]))
    if len(plan) > 1:
        whole = put(plan[:1], whole, quarters[:1])
        plan, quarters = plan[1:], quarters[1:]
    if plan:
        whole = put(plan, whole, quarters)
    return unview(whole, x, y)


def solution(mesh):
    placed = (
        P("mem", None, "tile", None),
        P(),
        P("tile"),
        P("mem", "tm", None, "tile", None),
        P("tm"),
        P("tm"),
    )
    return jax.shard_map(
        per_device,
        mesh=mesh,
        in_specs=placed,
        out_specs=P("tm", None, "tile", None),
        check_vma=False,
    )
```

```python
import functools
import math

import jax
import jax.numpy as jnp
from jax import lax
from jax.experimental import pallas as pl
from jax.experimental.pallas import tpu as pltpu
from jax.sharding import PartitionSpec as P


SMOOTH = 4
LANES = 128
ROWS = 8
VMEM_BYTES = 64 * 1024 * 1024

diffusion = 0.24


def ring(count, shift):
    return [(i, (i + shift) % count) for i in range(count)]


def is_power(count):
    return count & (count - 1) == 0


def pairing(count, step):
    if is_power(count):
        return [(i, i ^ step) for i in range(count)]
    return ring(count, step)


def target_of(place, count, step):
    if is_power(count):
        return place ^ step
    return lax.rem(place + step, count)


def stage_plan(stages):
    if stages == 4:
        return [[2, 3, 0, 1], [3, 2, 0, 1], [1, 0, 3, 2]]
    return [[(i + step) % stages for i in range(stages)] for step in range(1, stages)]


def plan_of(group):
    return [group - 1][: group - 1] + list(range(1, group - 1))


def source_of(place, count, step):
    if is_power(count):
        return place ^ step
    return lax.rem(place - step + count, count)


def view(field):
    lead = field.shape[:-3]
    levels, x, y = field.shape[-3:]
    field = field.reshape(*lead, levels, x, y // LANES, LANES)
    field = jnp.swapaxes(field, -3, -2)
    return field.reshape(*lead, levels * x * (y // LANES), LANES)


def flat(field):
    return view(field.reshape(-1, *field.shape[2:]))


def unview(rows, x, y):
    lead = rows.shape[:-2]
    tiles = y // LANES
    rows = rows.reshape(*lead, rows.shape[-2] // (x * tiles), tiles, x, LANES)
    rows = jnp.swapaxes(rows, -3, -2)
    return rows.reshape(*lead, -1, x, y)


def relax(field):
    neighbours = jnp.roll(field, -1, axis=2) + jnp.roll(field, 1, axis=2)
    bordered = jnp.pad(field, ((0, 0), (0, 0), (0, 0), (1, 1)))
    lateral = bordered[:, :, :, 2:] + bordered[:, :, :, :-2]
    return field + diffusion * (neighbours + lateral - 4.0 * field)


def smooth(field):
    count = lax.axis_size("tile")
    width = field.shape[2]
    left = SMOOTH
    while left:
        reach = min(left, width)
        head = lax.slice_in_dim(field, 0, reach, axis=2)
        tail = lax.slice_in_dim(field, width - reach, width, axis=2)
        before = lax.ppermute(tail, "tile", ring(count, 1))
        after = lax.ppermute(head, "tile", ring(count, -1))
        wide = jnp.concatenate([before, field, after], axis=2)
        for _ in range(reach):
            wide = relax(wide)
        field = lax.slice_in_dim(wide, reach, reach + width, axis=2)
        left -= reach
    return field


def load_kernel(
    x, modes_hbm, counts_hbm, index_hbm, weight_hbm, own_hbm,
    own_ref, splat_ref, mask_ref, factor_ref,
    modes_ref, counts_ref, index_ref, weight_ref, sems,
):
    pairs = [
        (modes_hbm, modes_ref),
        (counts_hbm, counts_ref),
        (index_hbm, index_ref),
        (weight_hbm, weight_ref),
        (own_hbm, own_ref),
    ]
    copies = [pltpu.make_async_copy(a, b, sems.at[i]) for i, (a, b) in enumerate(pairs)]
    for copy in copies:
        copy.start()
    for copy in copies[:-1]:
        copy.wait()
    levels, modes = splat_ref.shape[:2]
    for l in range(levels):
        for m in range(modes):
            splat_ref[l, m] = jnp.full((ROWS, LANES), modes_ref[m, l], jnp.float32)
    mode = lax.rem(lax.broadcasted_iota(jnp.int32, mask_ref.shape[1:], 0), modes)
    for i in range(x):
        mask_ref[i] = (mode < counts_ref[i]).astype(jnp.float32)
    windows, slots = factor_ref.shape[:2]
    for w in range(windows):
        local = index_ref[w] - lax.axis_index("tm") * slots
        for t in range(slots):
            factor = jnp.where(local == t, weight_ref[w], jnp.where(local > t, 1.0, 0.0))
            factor_ref[w, t] = jnp.full((ROWS, LANES), factor, jnp.float32)
    for copy in copies[-1:]:
        copy.wait()


def product(group, step, share, splat_ref, field_ref, part_ref, total_ref, lead_ref):
    members, slots = part_ref.shape[:2]
    modes = splat_ref.shape[1]
    owner = target_of(lax.axis_index("mem"), group, step)
    pair = 2 * ROWS
    for j in range(share // 2):
        level = owner * share + 2 * j
        start = pl.multiple_of(level * ROWS, pair)
        localized = []
        for k in range(members):
            halves = []
            for h in range(2):
                value = splat_ref[level + h, 0] * field_ref[pl.ds(k * modes * ROWS, ROWS), :]
                for m in range(1, modes):
                    value = value + splat_ref[level + h, m] * field_ref[pl.ds((k * modes + m) * ROWS, ROWS), :]
                halves.append(value)
            localized.append(jnp.concatenate(halves, axis=0))
        whole = None
        for t in range(slots):
            total = None
            for k in range(members):
                term = localized[k] * part_ref[k, t, pl.ds(start, pair), :].astype(jnp.float32)
                total = term if total is None else total + term
            if t < slots - 1:
                lead_ref[t, pl.ds(2 * j * ROWS, pair), :] = total
            whole = total if whole is None else whole + total
        total_ref[pl.ds(2 * j * ROWS, pair), :] = whole


def smooth_kernel(mask_ref, own_ref, other_ref, field_ref):
    x, pairs = mask_ref.shape[:2]
    tiles = ROWS // x
    cells = [
        [ref[pl.ds(tile * x + i, pairs, stride=ROWS), :] for tile in range(tiles)]
        for ref in (own_ref, other_ref)
        for i in range(x)
    ]
    lane = lax.broadcasted_iota(jnp.int32, (pairs, LANES), 1)
    first, last = lane == 0, lane == LANES - 1
    round_ = len(cells)
    for left in range(SMOOTH - 1, -1, -1):
        fresh = list(cells)
        for i in sorted({j % round_ for j in range(-left, x + left)}):
            up = [pltpu.roll(part, 1, 1) for part in cells[i]]
            down = [pltpu.roll(part, LANES - 1, 1) for part in cells[i]]
            fresh[i] = []
            for tile in range(tiles):
                before = up[tile - 1] if tile else 0.0
                after = down[tile + 1] if tile + 1 < tiles else 0.0
                near = jnp.where(first, before, up[tile]) + jnp.where(last, after, down[tile])
                near = near + (cells[i - 1][tile] + cells[(i + 1) % round_][tile])
                fresh[i].append((1.0 - 4.0 * diffusion) * cells[i][tile] + diffusion * near)
        cells = fresh
    for i in range(x):
        for tile in range(tiles):
            field_ref[pl.ds(tile * x + i, pairs, stride=ROWS), :] = cells[i][tile] * mask_ref[i]


def mask_kernel(mask_ref, own_ref, field_ref):
    x, pairs = mask_ref.shape[:2]
    for i in range(ROWS):
        rows = pl.ds(i, pairs, stride=ROWS)
        field_ref[rows, :] = own_ref[rows, :] * mask_ref[i % x]


def gather_kernel(norm_factor, *refs):
    *arrived, out_ref = refs
    value = arrived[0][...]
    for ref in arrived[1:]:
        value = value + ref[...]
    out_ref[...] = value * norm_factor


def scale_kernel(norm_factor, lead_ref, out_ref):
    out_ref[...] = lead_ref[...] * norm_factor


def slots_kernel(norm_factor, total_ref, own_ref, *refs):
    *leads, slots_ref = refs
    slots = slots_ref.shape[0]
    rest = total_ref[...]
    for t in range(slots - 1):
        value = own_ref[t]
        for ref in leads:
            value = value + ref[t] * norm_factor
        slots_ref[t] = value
        rest = rest - value
    slots_ref[slots - 1] = rest


def mix_kernel(factor_ref, slots_ref, out_ref):
    windows, height = out_ref.shape[:2]
    for r in range(0, height, ROWS):
        rows = slice(r, r + ROWS)
        for w in range(windows):
            mixed = factor_ref[w, 0] * slots_ref[0, rows]
            for t in range(1, slots_ref.shape[0]):
                mixed = mixed + factor_ref[w, t] * slots_ref[t, rows]
            out_ref[w, rows] = mixed


def earlier_kernel(stages, *refs):
    *arrived, earlier_ref = refs
    stage = lax.axis_index("tm")
    earlier = jnp.zeros(earlier_ref.shape, jnp.float32)
    for targets, ref in zip(stage_plan(stages), arrived):
        ahead = jnp.float32(0.0)
        for source, target in enumerate(targets):
            if source < target:
                ahead = jnp.where(stage == target, 1.0, ahead)
        earlier = earlier + ref[...] * ahead
    earlier_ref[...] = earlier


def copies_out(group, step, part_ref, out_ref, sems):
    windows, height = part_ref.shape[:2]
    owner = source_of(lax.axis_index("mem"), group, step)
    start = pl.multiple_of(owner * height, height)
    return [
        pltpu.make_async_copy(part_ref.at[w], out_ref.at[w, pl.ds(start, height)], sems.at[w])
        for w in range(windows)
    ]


def place_kernel(group, plan, goes_on, *refs):
    refs = list(refs)
    if goes_on:
        refs.pop(0)
    quarters = [(refs.pop(0), refs.pop(0)) for _ in plan]
    out_ref, *parts, sems = refs
    copies = []
    for i, (step, (mixed_ref, earlier_ref), part_ref) in enumerate(zip(plan, quarters, parts)):
        started = copies_out(group, step, part_ref, out_ref, sems.at[i])
        for w, copy in enumerate(started):
            part_ref[w] = mixed_ref[w] + earlier_ref[...]
            copy.start()
        copies += started
    for copy in copies:
        copy.wait()


VMEM_SPEC = pl.BlockSpec(memory_space=pltpu.VMEM)
HBM_SPEC = pl.BlockSpec(memory_space=pltpu.HBM)


def call(kernel, arrays, out_shape, cost):
    return pl.pallas_call(
        kernel,
        in_specs=[VMEM_SPEC] * len(arrays),
        out_specs=jax.tree.map(lambda _: VMEM_SPEC, out_shape),
        out_shape=out_shape,
        compiler_params=pltpu.CompilerParams(vmem_limit_bytes=16 * 1024 * 1024),
        cost_estimate=pl.CostEstimate(flops=cost, bytes_accessed=cost, transcendentals=0),
    )(*arrays)


def per_device(control, vertical_modes, mode_counts, perturbations, slot_index, blend_weight):
    members, slot_count, levels, x, y = perturbations.shape
    modes = vertical_modes.shape[1]
    windows = slot_index.shape[0]
    group = lax.axis_size("mem")
    stages = lax.axis_size("tm")
    share = levels // group
    height = share * ROWS
    norm_factor = 1.0 / math.sqrt(members * group - 1)
    f32 = lambda *shape: jax.ShapeDtypeStruct(shape, jnp.float32)
    parts = view(perturbations)
    own = flat(control)

    room = parts.size * parts.dtype.itemsize + levels * modes * ROWS * LANES * 4

    loaded, splats, masks, factors = pl.pallas_call(
        functools.partial(load_kernel, x),
        in_specs=[HBM_SPEC] * 5,
        out_specs=[VMEM_SPEC] * 4,
        out_shape=[
            pltpu.VMEM(own.shape, jnp.float32),
            pltpu.VMEM((levels, modes, ROWS, LANES), jnp.float32),
            pltpu.VMEM((x, members * modes, LANES), jnp.float32),
            pltpu.VMEM((windows, slot_count, ROWS, LANES), jnp.float32),
        ],
        scratch_shapes=[
            pltpu.SMEM((modes, levels), jnp.float32),
            pltpu.SMEM(mode_counts.shape, jnp.int32),
            pltpu.SMEM(slot_index.shape, jnp.int32),
            pltpu.SMEM(blend_weight.shape, jnp.float32),
            pltpu.SemaphoreType.DMA((5,)),
        ],
        compiler_params=pltpu.CompilerParams(vmem_limit_bytes=VMEM_BYTES - 2 * room),
        cost_estimate=pl.CostEstimate(flops=1000000000, bytes_accessed=1000000000, transcendentals=0),
    )(vertical_modes.T, mode_counts, slot_index, blend_weight, own)

    shapes = [f32(height, LANES), f32(slot_count - 1, height, LANES)]
    field_shape = f32(members * modes * ROWS, LANES)
    plan = plan_of(group)
    if lax.axis_size("tile") == 2 and x == SMOOTH:
        other = lax.ppermute(control, "tile", ring(2, 1))
        field = call(
            smooth_kernel, [masks, loaded, flat(other)], field_shape, 1000
        )
    else:
        field = call(mask_kernel, [masks, flat(smooth(control))], field_shape, 1000)

    products = []
    for step in plan + [0]:
        products.append(
            call(
                functools.partial(product, group, step, share),
                [splats, field, parts],
                shapes,
                1000000,
            )
        )

    totals, leads = [products[-1][0]], [products[-1][1]]
    for i, step in enumerate(plan):
        totals.append(lax.ppermute(products[i][0], "mem", pairing(group, step)))
        leads.append(lax.ppermute(products[i][1], "mem", pairing(group, step)))
    total = call(functools.partial(gather_kernel, norm_factor), totals, f32(height, LANES), 1000000)

    came = []
    for targets in stage_plan(stages):
        came.append(lax.ppermute(total, "tm", list(enumerate(targets))))
    scaled = call(
        functools.partial(scale_kernel, norm_factor), [leads[0]], shapes[1], 1000000
    )
    slots = call(
        functools.partial(slots_kernel, norm_factor),
        [total, scaled] + leads[1:],
        f32(slot_count, height, LANES),
        1000000,
    )
    slots_far = []
    for step in plan:
        slots_far.append(lax.ppermute(slots, "mem", pairing(group, step)))
    mixed = call(mix_kernel, [factors, slots], f32(windows, height, LANES), 1000000)
    earlier = call(
        functools.partial(earlier_kernel, stages), came, f32(height, LANES), 1000000
    )
    earlier_far = []
    for step in plan:
        earlier_far.append(lax.ppermute(earlier, "mem", pairing(group, step)))

    def put(steps, whole, quarters):
        first = [] if whole is None else [whole]
        return pl.pallas_call(
            functools.partial(place_kernel, group, steps, bool(first)),
            in_specs=[HBM_SPEC] * len(first) + [VMEM_SPEC] * (2 * len(steps)),
            out_specs=HBM_SPEC,
            out_shape=pltpu.HBM((windows, levels * ROWS, LANES), jnp.float32),
            scratch_shapes=[pltpu.VMEM((windows, height, LANES), jnp.float32)] * len(steps)
            + [pltpu.SemaphoreType.DMA((len(steps), windows))],
            input_output_aliases={0: 0} if first else {},
            compiler_params=pltpu.CompilerParams(vmem_limit_bytes=16 * 1024 * 1024),
            cost_estimate=pl.CostEstimate(flops=1000000, bytes_accessed=0, transcendentals=0),
        )(*first, *[ref for pair in quarters for ref in pair])

    whole = put([0], None, [(mixed, earlier)])
    quarters = []
    for i, part in enumerate(slots_far):
        part = call(mix_kernel, [factors, part], f32(windows, height, LANES), 1000000)
        quarters.append((part, earlier_far[i]))
    if len(plan) > 1:
        whole = put(plan[:1], whole, quarters[:1])
        plan, quarters = plan[1:], quarters[1:]
    if plan:
        whole = put(plan, whole, quarters)
    return unview(whole, x, y)


def solution(mesh):
    placed = (
        P("mem", None, "tile", None),
        P(),
        P("tile"),
        P("mem", "tm", None, "tile", None),
        P("tm"),
        P("tm"),
    )
    return jax.shard_map(
        per_device,
        mesh=mesh,
        in_specs=placed,
        out_specs=P("tm", None, "tile", None),
        check_vma=False,
    )
```
